1024 devices in a mesh: sp: 32 (over y, x, core), dp: 32 (over z).
Axes of the slice: x: 4, y: 4, z: 32, core: 2. Of those that a mesh axis runs over, the one named last changes fastest.
Arguments:
- hidden: bfloat16 [32, 8192, 4096], P('dp', 'sp'), may hold values from -24 to 24
- pad_counts: int32 [32, 32], P('dp', 'sp'), may hold values from 64 to 128
- doc_lengths: int32 [32, 128], P('dp'), may hold values from 1 to 128, 8192 in all within a row
- range_shift: int32 [32, 32], P('dp'), may hold values from -32 to 32
- qkv_weight: bfloat16 [4096, 384], P('dp'), may hold values from -0.09375 to 0.09375
Outputs:
- attended: bfloat16 [32, 8192, 128], P('dp', 'sp')
The draws below stay inside these ranges and needn't reach their ends.
Inputs may be any that keep to these rules, and one draw needn't show every extreme that they name: `doc_lengths`: each row sums to 8192.
All inputs are finite; a program needn't handle non-finite values.
Results may differ from the reference program's by a relative error of at most 0.0095.
Values may be sent and summed in bfloat16 or wider, within the bound.
No kernel may reach another device: no remote copies, remote signals or barrier semaphores. Data moves between devices by JAX's collectives and lax.ppermute only.
A program may use at most 32 MiB of HBM per device.

```python
import math
import jax
import jax.numpy as jnp
import numpy as np
from jax import lax

D = 4096
HEAD_DIM = 128
ROWS_DEV = 256
MICRO = 32
SLOTS = 8192
DOCS = 128
N_SP = 32
N_DP = 32


def draw_hidden(key, part):
    normal_rows = jnp.clip(jax.random.normal(key, (MICRO, SLOTS, D), jnp.float32), -6.0, 6.0)
    return normal_rows.astype(jnp.bfloat16)


def with_ends(entries, own_key, least, top_value):
    longest = entries.shape.index(max(entries.shape))
    spots = []
    for shift in (0, 1):
        where = [jax.random.randint(jax.random.fold_in(own_key, axis), (), 0, length) for axis, length in enumerate(entries.shape)]
        where[longest] = (where[longest] + shift) % entries.shape[longest]
        spots.append(tuple(where))
    return entries.at[spots[0]].set(least).at[spots[1]].set(top_value)


def levels(stream_key, extent, shards, least, top_value):
    loudness, own = 1.0, jax.random.fold_in(stream_key, 6)
    for axis_at, blocks in shards:
        draws = jnp.exp(jax.random.uniform(jax.random.fold_in(own, axis_at), (blocks,), jnp.float32, least / len(shards), top_value / len(shards)))
        loudness = loudness * jnp.repeat(draws, extent[axis_at] // blocks).reshape([-1 if axis == axis_at else 1 for axis in range(len(extent))])
    return loudness


def split_up(count, total, reach, lean):
    portions = [(1 << 20) // math.isqrt(grade ** lean) + 1 for grade in range(2, count + 1)]
    spare, given = total - reach - (count - 1), [1] * (count - 1)
    while spare > 0:
        movable = [i for i in range(count - 1) if given[i] < reach]
        mass, remaining = sum([portions[i] for i in movable]), spare
        for i in movable:
            more = min(reach - given[i], max(1, remaining * portions[i] // mass), spare)
            given[i] = given[i] + more
            spare = spare - more
    return np.array([reach] + given)


def ragged(own_key, number_of, total, bound, skew):
    if number_of == 2:
        one = jax.random.randint(own_key, (), max(1, total - bound), min(bound, total - 1) + 1)
        return jnp.stack([one, total - one])
    tallies = jnp.asarray(split_up(number_of, total, bound, skew), jnp.int32)
    twos = (number_of - 1) // 2
    donor, receiver = tallies[1:1 + 2 * twos:2], tallies[2:2 + 2 * twos:2]
    margin = jnp.minimum(donor - 1, bound - receiver)
    shifted = jax.random.randint(jax.random.fold_in(own_key, 1), (twos,), 0, 1 << 20) % (margin + 1)
    tallies = tallies.at[1:1 + 2 * twos:2].set(donor - shifted).at[2:2 + 2 * twos:2].set(receiver + shifted)
    return tallies[jax.random.permutation(jax.random.fold_in(own_key, 2), number_of)]


def centred(key, shape, deviation, most, cuts=(), kind=jnp.bfloat16):
    array = jax.random.normal(key, shape, jnp.float32) * deviation
    if len(cuts) > 0:
        array = levels(key, shape, cuts, -0.22, 0.18) * array
    return jnp.clip(array, min=-most, max=most).astype(kind)


def setup_inputs(seed: int = 0) -> dict:
    seeds = jax.random.split(jax.random.key(seed), 6)
    return {
        "hidden": draw_hidden(jax.random.fold_in(seeds[5], 71), 0),
        "pad_counts": with_ends(jax.random.randint(seeds[1], (MICRO, N_SP), ROWS_DEV // 4, ROWS_DEV // 2 + 1), jax.random.fold_in(seeds[1], 1), ROWS_DEV // 4, (ROWS_DEV // 2 + 1) - 1).astype(jnp.int32),
        "doc_lengths": jax.vmap(lambda own: ragged(own, DOCS, SLOTS, ROWS_DEV // 2, 1))(jax.random.split(seeds[2], MICRO)).reshape((MICRO, DOCS)).astype(jnp.int32),
        "range_shift": with_ends(jax.random.randint(seeds[3], (MICRO, N_SP), 0 - ROWS_DEV // 8, ROWS_DEV // 8 + 1), jax.random.fold_in(seeds[3], 1), 0 - ROWS_DEV // 8, (ROWS_DEV // 8 + 1) - 1).astype(jnp.int32),
        "qkv_weight": centred(seeds[4], (D, 3 * HEAD_DIM), D ** -0.5, 0.09375, ((0, 32),)),
    }


def attend_block(projected, position, row_live, doc_ids):
    head_dim = projected.shape[1] // 3
    query = projected[:, :head_dim].astype(jnp.float32)
    keys = projected[:, head_dim:2 * head_dim].astype(jnp.float32)
    values = projected[:, 2 * head_dim:].astype(jnp.float32)
    scores = jnp.einsum('qd,kd->qk', query, keys) / math.sqrt(head_dim)
    allowed = (doc_ids[:, None] == doc_ids[None, :]) & (position[None, :] <= position[:, None])
    allowed = allowed & row_live[:, None] & row_live[None, :]
    masked = jnp.where(allowed, scores, -1e+30)
    row_peak = lax.optimization_barrier(jnp.max(masked, axis=1, keepdims=True))
    exponent = jnp.where(allowed, jnp.exp(masked - row_peak), 0.0)
    denominator = lax.optimization_barrier(jnp.sum(exponent, axis=1, keepdims=True))
    attention_probs = (exponent / jnp.where(row_live[:, None], denominator, 1.0)).astype(jnp.bfloat16)
    result = jnp.einsum('qk,kd->qd', attention_probs.astype(jnp.float32), values)
    return jnp.where(row_live[:, None], result, 0.0).astype(jnp.bfloat16)

def reference(hidden, pad_counts, doc_lengths, range_shift, qkv_weight):

    def one_micro(operands):
        slot_rows, padding, lengths, shifts = operands
        live_count = (ROWS_DEV - padding).astype(jnp.int32)
        token_start = (jnp.cumsum(live_count) - live_count).astype(jnp.int32)
        total_tokens = (token_start[-1] + live_count[-1]).astype(jnp.int32)
        range_first = jnp.concatenate([jnp.zeros((1,), jnp.int32), (token_start[1:] + shifts[1:]).astype(jnp.int32)])
        range_end = jnp.concatenate([range_first[1:], total_tokens[None]]).astype(jnp.int32)
        local_rows = jnp.arange(ROWS_DEV, dtype=jnp.int32)
        position = (range_first[:, None] + local_rows[None, :]).astype(jnp.int32)
        row_live = local_rows[None, :] < (range_end - range_first)[:, None]
        device_of = (lax.optimization_barrier(jnp.sum((token_start[None, None, :] <= position[:, :, None]).astype(jnp.int32), axis=2)) - 1).astype(jnp.int32)
        slot_of = (jnp.take(padding, device_of) + position - jnp.take(token_start, device_of)).astype(jnp.int32)
        flat_slot = jnp.clip(device_of * ROWS_DEV + slot_of, 0, N_SP * ROWS_DEV - 1).astype(jnp.int32)
        gathered = jnp.take(slot_rows, flat_slot.reshape(-1), axis=0).reshape(N_SP, ROWS_DEV, D)
        owned_rows = jnp.where(row_live[:, :, None], gathered, 0).astype(jnp.bfloat16)
        projected = jnp.dot(owned_rows.reshape(N_SP * ROWS_DEV, D), qkv_weight, preferred_element_type=jnp.float32)
        projected = projected.astype(jnp.bfloat16).reshape(N_SP, ROWS_DEV, 3 * HEAD_DIM)
        doc_ends = jnp.cumsum(lengths).astype(jnp.int32)
        doc_ids = lax.optimization_barrier(jnp.sum((doc_ends[None, None, :] <= position[:, :, None]).astype(jnp.int32), axis=2)).astype(jnp.int32)
        return jax.vmap(attend_block)(projected, position, row_live, doc_ids)
    blocks = lax.map(one_micro, (hidden, pad_counts, doc_lengths, range_shift))
    return blocks.reshape(N_DP, N_SP * ROWS_DEV, HEAD_DIM)
```

```python
import functools
import math

import jax
import jax.numpy as jnp
from jax import lax
from jax.experimental import pallas as pl
from jax.experimental.pallas import tpu as pltpu
from jax.sharding import Mesh
from jax.sharding import PartitionSpec as P

PLANE = ("y", "x", "core")
EDGE = 32
CHUNK = 512
SMALL = pltpu.CompilerParams(vmem_limit_bytes=16 * 1024 * 1024)


def gather_kernel(scalars, slots, left, right, owned):
    rows = slots.shape[0]
    padding, live, shift, count = (scalars[i] for i in range(4))
    row = lax.broadcasted_iota(jnp.int32, (rows, 1), 0)
    offset = row + shift
    slot = jnp.where(
        offset < 0,
        rows + EDGE + offset,
        jnp.where(offset < live, padding + offset, rows + EDGE + offset - live),
    )
    slot = jnp.where(row < count, slot, -1)
    here = lax.broadcasted_iota(jnp.int32, (rows, rows), 1)
    edge = lax.broadcasted_iota(jnp.int32, (rows, 2 * EDGE), 1) + rows
    pick_here = jnp.where(here == slot, 1.0, 0.0).astype(jnp.bfloat16)
    pick_edge = jnp.where(edge == slot, 1.0, 0.0).astype(jnp.bfloat16)
    for at in range(0, slots.shape[1], CHUNK):
        columns = slice(at, at + CHUNK)
        edges = jnp.concatenate([left[:, columns], right[:, columns]], axis=0)
        owned[:, columns] = (
            jnp.dot(pick_here, slots[:, columns], preferred_element_type=jnp.float32)
            + jnp.dot(pick_edge, edges, preferred_element_type=jnp.float32)
        ).astype(jnp.bfloat16)


def gather_rows(scalars, slots, left, right):
    rows, width = slots.shape
    return pl.pallas_call(
        gather_kernel,
        out_shape=jax.ShapeDtypeStruct((rows, width), jnp.bfloat16),
        in_specs=[pl.BlockSpec(memory_space=pltpu.SMEM)]
        + [pl.BlockSpec(memory_space=pltpu.VMEM)] * 3,
        out_specs=pl.BlockSpec(memory_space=pltpu.VMEM),
        cost_estimate=pl.CostEstimate(
            flops=2 * rows * (rows + 2 * EDGE) * width,
            bytes_accessed=4 * rows * width,
            transcendentals=0,
        ),
        compiler_params=SMALL,
        name="gather_rows",
    )(scalars, slots, left, right)


def weave_kernel(core, half, other, weight):
    chips, heads, parts = half.shape[:3]

    def one(part, carry):
        for at in range(chips):
            for head in range(heads):
                weight[head, part, 2 * at + core[0]] = half[at, head, part]
                weight[head, part, 2 * at + 1 - core[0]] = other[at, head, part]
        return carry

    lax.fori_loop(0, parts, one, 0)


def weave(core, half, other):
    chips, heads, parts, deep, lanes = half.shape
    return pl.pallas_call(
        weave_kernel,
        out_shape=jax.ShapeDtypeStruct((heads, parts, 2 * chips, deep, lanes), jnp.bfloat16),
        in_specs=[pl.BlockSpec(memory_space=pltpu.SMEM)]
        + [pl.BlockSpec(memory_space=pltpu.VMEM)] * 2,
        out_specs=pl.BlockSpec(memory_space=pltpu.VMEM),
        compiler_params=SMALL,
        name="weave",
    )(core, half, other)


def attend_kernel(scalars, owned, weight, ends, attended):
    rows = owned.shape[0]
    head_dim = attended.shape[1]
    start, count = scalars[0], scalars[1]
    pair = jnp.concatenate([weight[0], weight[1]], axis=1)
    both = jnp.dot(owned[...], pair, preferred_element_type=jnp.float32).astype(jnp.bfloat16)
    values = jnp.dot(owned[...], weight[2], preferred_element_type=jnp.float32).astype(
        jnp.bfloat16
    )
    query, keys = both[:, :head_dim], both[:, head_dim:]
    scores = lax.dot_general(
        query, keys, (((1,), (1,)), ((), ())), preferred_element_type=jnp.float32
    ) / math.sqrt(head_dim)
    row = lax.broadcasted_iota(jnp.int32, (rows, 1), 0)
    key = lax.broadcasted_iota(jnp.int32, (rows, rows), 1)
    passed = jnp.where(ends[...] <= row + start, ends[...], 0)
    opened = jnp.max(passed, axis=1, keepdims=True) - start
    live = row < count
    allowed = (key <= row) & (key >= opened) & live
    masked = jnp.where(allowed, scores, -1e30)
    peak = jnp.max(masked, axis=1, keepdims=True)
    exponent = jnp.where(allowed, jnp.exp(masked - peak), 0.0)
    denominator = jnp.sum(exponent, axis=1, keepdims=True)
    probs = (exponent / jnp.where(live, denominator, 1.0)).astype(jnp.bfloat16)
    result = jnp.dot(probs, values, preferred_element_type=jnp.float32)
    attended[...] = jnp.where(live, result, 0.0).astype(jnp.bfloat16)


def attend(scalars, owned, weight, ends):
    rows, head_dim = owned.shape[0], weight.shape[2]
    return pl.pallas_call(
        attend_kernel,
        out_shape=jax.ShapeDtypeStruct((rows, head_dim), jnp.bfloat16),
        in_specs=[pl.BlockSpec(memory_space=pltpu.SMEM)]
        + [pl.BlockSpec(memory_space=pltpu.VMEM)] * 3,
        out_specs=pl.BlockSpec(memory_space=pltpu.VMEM),
        compiler_params=SMALL,
        name="attend",
    )(scalars, owned, weight, ends)


def for_each(value, count):
    return jnp.broadcast_to(value[None], (count, *value.shape))


def weight_column(own):
    index = lax.axis_index(PLANE)
    deep = own.shape[0] // lax.axis_size(PLANE)
    lanes = own.shape[1] // 3
    piece = lax.dynamic_slice_in_dim(own, index * deep, deep, 0)
    piece = piece.reshape(deep, 3, lanes).transpose(1, 0, 2)
    column = lax.all_to_all(for_each(piece, lax.axis_size("z")), "z", 0, 0, tiled=True)
    return column.transpose(1, 0, 2, 3)


def shards(hidden, pad_counts, doc_lengths, range_shift, qkv_weight):
    slots = hidden[0]
    rows = slots.shape[0]
    size, index = lax.axis_size(PLANE), lax.axis_index(PLANE)
    padding = pad_counts[0, 0]
    live = rows - padding

    column = weight_column(qkv_weight)

    head = lax.dynamic_slice_in_dim(slots, padding, EDGE, 0)
    tail = slots[rows - EDGE :]
    left = lax.ppermute(tail, PLANE, [(i, i + 1) for i in range(size - 1)])
    right = lax.ppermute(head, PLANE, [(i + 1, i) for i in range(size - 1)])
    counts = lax.all_to_all(
        jnp.broadcast_to(live, (size, 1)), PLANE, 0, 0, tiled=True
    )[:, 0]
    column, counts = lax.optimization_barrier((column, counts))

    chips = lax.axis_size(("y", "x"))
    half = lax.all_to_all(for_each(column, chips), ("y", "x"), 0, 0, tiled=True)

    token_start = jnp.sum(jnp.where(jnp.arange(size) < index, counts, 0))
    shifts = range_shift[0]
    shift = jnp.where(index == 0, 0, shifts[index])
    following = jnp.where(index == size - 1, 0, shifts[jnp.minimum(index + 1, size - 1)])
    count = live + following - shift
    scalars = jnp.stack([padding, live, shift, count]).astype(jnp.int32)
    owned = gather_rows(scalars, slots, left, right)
    ends = jnp.cumsum(doc_lengths[0])[None]
    where = jnp.stack([token_start + shift, count]).astype(jnp.int32)
    half, owned, ends, where = lax.optimization_barrier((half, owned, ends, where))

    other = lax.ppermute(half, "core", [(0, 1), (1, 0)])
    core = lax.axis_index("core").reshape(1)
    weight = weave(core, half, other)
    weight = weight.reshape(3, -1, weight.shape[-1])
    return attend(where, owned, weight, ends)[None]


def solution(mesh):
    fine = Mesh(mesh.devices.reshape(4, 4, 2, -1), ("y", "x", "core", "z"))
    in_specs = (P("z", PLANE, None), P("z", PLANE), P("z", None), P("z", None), P("z", None))
    return jax.shard_map(
        shards, mesh=fine, in_specs=in_specs, out_specs=P("z", PLANE, None), check_vma=False
    )
```

```python
import math

import jax
import jax.numpy as jnp
from jax import lax
from jax.experimental import pallas as pl
from jax.experimental.pallas import tpu as pltpu
from jax.sharding import Mesh
from jax.sharding import PartitionSpec as P

PLANE = ("y", "x", "core")
EDGE = 32
NEAR = [d for k in range(8) for _ in range(2) for d in ((k, -k) if k else (0, 8))]
FAR = [d for k in range(8) for _ in range(2) for d in ((16 - k, k - 16) if k else (16, -8))]
SHIFTS = (NEAR, FAR)
CHUNK = 512
SMALL = pltpu.CompilerParams(vmem_limit_bytes=16 * 1024 * 1024)


def gather_kernel(scalars, slots, left, right, owned):
    rows = slots.shape[0]
    padding, live, shift, count = (scalars[i] for i in range(4))
    row = lax.broadcasted_iota(jnp.int32, (rows, 1), 0)
    offset = row + shift
    slot = jnp.where(
        offset < 0,
        rows + EDGE + offset,
        jnp.where(offset < live, padding + offset, rows + EDGE + offset - live),
    )
    slot = jnp.where(row < count, slot, -1)
    here = lax.broadcasted_iota(jnp.int32, (rows, rows), 1)
    edge = lax.broadcasted_iota(jnp.int32, (rows, 2 * EDGE), 1) + rows
    pick_here = jnp.where(here == slot, 1.0, 0.0).astype(jnp.bfloat16)
    pick_edge = jnp.where(edge == slot, 1.0, 0.0).astype(jnp.bfloat16)
    for at in range(0, slots.shape[1], CHUNK):
        columns = slice(at, at + CHUNK)
        edges = jnp.concatenate([left[:, columns], right[:, columns]], axis=0)
        owned[:, columns] = (
            jnp.dot(pick_here, slots[:, columns], preferred_element_type=jnp.float32)
            + jnp.dot(pick_edge, edges, preferred_element_type=jnp.float32)
        ).astype(jnp.bfloat16)


def gather_rows(scalars, slots, left, right):
    rows, width = slots.shape
    return pl.pallas_call(
        gather_kernel,
        out_shape=jax.ShapeDtypeStruct((rows, width), jnp.bfloat16),
        in_specs=[pl.BlockSpec(memory_space=pltpu.SMEM)]
        + [pl.BlockSpec(memory_space=pltpu.VMEM)] * 3,
        out_specs=pl.BlockSpec(memory_space=pltpu.VMEM),
        cost_estimate=pl.CostEstimate(
            flops=2 * rows * (rows + 2 * EDGE) * width,
            bytes_accessed=4 * rows * width,
            transcendentals=0,
        ),
        compiler_params=SMALL,
        name="gather_rows",
    )(scalars, slots, left, right)


def attend_kernel(scalars, owned, half, other, ends, attended, weight):
    rows = owned.shape[0]
    head_dim = attended.shape[1]
    shift, count, core, plane, index = (scalars[i] for i in range(5))
    chips, tiles = half.shape[0], half.shape[1] // 2
    planes, deep = chips * 2, tiles // 3
    before = jnp.zeros(half.shape[2:], jnp.float32)
    for chip in range(chips):
        for side, block in ((core, half), (1 - core, other)):
            for kind in range(2):
                north, south = (SHIFTS[kind][2 * chip + c] for c in range(2))
                shard = lax.rem(plane + planes - jnp.where(side == 0, north, south), planes)
                for at in range(deep):
                    for part in range(3):
                        weight[part, 2 * shard + chip % 2, at] = block[
                            chip, kind * tiles + at * 3 + part
                        ]
            before += jnp.where(
                2 * chip + side < index, block[chip, 2 * tiles].astype(jnp.float32), 0.0
            )
    start = before[:1, :1].astype(jnp.int32) + shift
    flat = jnp.concatenate(
        [weight[part].reshape(-1, head_dim) for part in range(3)], axis=1
    )
    projected = jnp.dot(owned[...], flat, preferred_element_type=jnp.float32).astype(
        jnp.bfloat16
    )
    query, keys, values = (projected[:, i * head_dim : (i + 1) * head_dim] for i in range(3))
    scores = lax.dot_general(
        query, keys, (((1,), (1,)), ((), ())), preferred_element_type=jnp.float32
    ) / math.sqrt(head_dim)
    row = lax.broadcasted_iota(jnp.int32, (rows, 1), 0)
    key = lax.broadcasted_iota(jnp.int32, (rows, rows), 1)
    passed = jnp.where(ends[...] <= row + start, ends[...], 0)
    opened = jnp.max(passed, axis=1, keepdims=True) - start
    live = row < count
    allowed = (key <= row) & (key >= opened) & live
    masked = jnp.where(allowed, scores, -1e30)
    peak = jnp.max(masked, axis=1, keepdims=True)
    exponent = jnp.where(allowed, jnp.exp(masked - peak), 0.0)
    denominator = jnp.sum(exponent, axis=1, keepdims=True)
    probs = (exponent / jnp.where(live, denominator, 1.0)).astype(jnp.bfloat16)
    result = jnp.dot(probs, values, preferred_element_type=jnp.float32)
    attended[...] = jnp.where(live, result, 0.0).astype(jnp.bfloat16)


def attend(scalars, owned, half, other, ends):
    chips, tiles, deep, lanes = half.shape
    return pl.pallas_call(
        attend_kernel,
        out_shape=jax.ShapeDtypeStruct((owned.shape[0], lanes), jnp.bfloat16),
        in_specs=[pl.BlockSpec(memory_space=pltpu.SMEM)]
        + [pl.BlockSpec(memory_space=pltpu.VMEM)] * 4,
        out_specs=pl.BlockSpec(memory_space=pltpu.VMEM),
        scratch_shapes=[pltpu.VMEM((3, 4 * chips, tiles // 6, deep, lanes), jnp.bfloat16)],
        compiler_params=SMALL,
        name="attend",
    )(scalars, owned, half, other, ends)


def for_each(value, count):
    return jnp.broadcast_to(value[None], (count, *value.shape))


def moved(value, kind):
    planes = lax.axis_size("z")
    pairs = [
        (j * planes + z, j * planes + (z + shift) % planes)
        for j, shift in enumerate(SHIFTS[kind])
        for z in range(planes)
    ]
    return lax.ppermute(value, (*PLANE, "z"), pairs)


def shards(hidden, pad_counts, doc_lengths, range_shift, qkv_weight):
    slots = hidden[0]
    rows = slots.shape[0]
    size, index = lax.axis_size(PLANE), lax.axis_index(PLANE)
    padding = pad_counts[0, 0]
    live = rows - padding

    deep = qkv_weight.shape[0] // 2
    own = lax.dynamic_slice_in_dim(qkv_weight, lax.axis_index("x") % 2 * deep, deep, 0)
    own = own.reshape(deep // 8, 8, 3, -1).transpose(0, 2, 1, 3)
    own = own.reshape(deep // 8 * 3, 8, -1)
    far = moved(own, 1)
    head = lax.dynamic_slice_in_dim(slots, padding, EDGE, 0)
    tail = slots[rows - EDGE :]
    left = lax.ppermute(tail, PLANE, [(i, i + 1) for i in range(size - 1)])
    right = lax.ppermute(head, PLANE, [(i + 1, i) for i in range(size - 1)])
    near = moved(own, 0)

    chips = lax.axis_size(("y", "x"))
    tally = jnp.full((1, *own.shape[1:]), live).astype(jnp.bfloat16)
    half = lax.all_to_all(
        for_each(jnp.concatenate([near, far, tally]), chips), ("y", "x"), 0, 0, tiled=True
    )
    shifts = range_shift[0]
    shift = jnp.where(index == 0, 0, shifts[index])
    following = jnp.where(index == size - 1, 0, shifts[jnp.minimum(index + 1, size - 1)])
    count = live + following - shift
    scalars = jnp.stack([padding, live, shift, count]).astype(jnp.int32)
    owned = gather_rows(scalars, slots, left, right)
    ends = jnp.cumsum(doc_lengths[0])[None]
    where = jnp.stack(
        [shift, count, lax.axis_index("core"), lax.axis_index("z"), index]
    ).astype(jnp.int32)
    half, owned, ends, where = lax.optimization_barrier((half, owned, ends, where))

    other = lax.ppermute(half, "core", [(0, 1), (1, 0)])
    return attend(where, owned, half, other, ends)[None]


def solution(mesh):
    fine = Mesh(mesh.devices.reshape(4, 4, 2, -1), ("y", "x", "core", "z"))
    in_specs = (P("z", PLANE, None), P("z", PLANE), P("z", None), P("z", None), P("z", None))
    return jax.shard_map(
        shards, mesh=fine, in_specs=in_specs, out_specs=P("z", PLANE, None), check_vma=False
    )
```

```python
import math

import jax
import jax.numpy as jnp
from jax import lax
from jax.experimental import pallas as pl
from jax.experimental.pallas import tpu as pltpu
from jax.sharding import Mesh
from jax.sharding import PartitionSpec as P

PLANE = ("y", "x", "core")
EDGE = 32
NEAR = [d for k in range(8) for _ in range(2) for d in ((k, -k) if k else (0, 8))]
FAR = [d for k in range(8) for _ in range(2) for d in ((16 - k, k - 16) if k else (16, -8))]
SHIFTS = (NEAR, FAR)
CHUNK = 512
LANES = 128
SMALL = pltpu.CompilerParams(vmem_limit_bytes=16 * 1024 * 1024)


def gather_kernel(scalars, slots, left, right, owned):
    rows = slots.shape[0]
    padding, live, shift, count = (scalars[i] for i in range(4))
    row = lax.broadcasted_iota(jnp.int32, (rows, 1), 0)
    offset = row + shift
    slot = jnp.where(
        offset < 0,
        rows + EDGE + offset,
        jnp.where(offset < live, padding + offset, rows + EDGE + offset - live),
    )
    slot = jnp.where(row < count, slot, -1)
    here = lax.broadcasted_iota(jnp.int32, (rows, rows), 1)
    edge = lax.broadcasted_iota(jnp.int32, (rows, 2 * EDGE), 1) + rows
    pick_here = jnp.where(here == slot, 1.0, 0.0).astype(jnp.bfloat16)
    pick_edge = jnp.where(edge == slot, 1.0, 0.0).astype(jnp.bfloat16)
    for at in range(0, slots.shape[1], CHUNK):
        columns = slice(at, at + CHUNK)
        edges = jnp.concatenate([left[:, columns], right[:, columns]], axis=0)
        picked = (
            jnp.dot(pick_here, slots[:, columns], preferred_element_type=jnp.float32)
            + jnp.dot(pick_edge, edges, preferred_element_type=jnp.float32)
        ).astype(jnp.bfloat16)
        for lane in range(0, CHUNK, LANES):
            owned[(at + lane) // LANES] = picked[:, lane : lane + LANES]


def gather_rows(scalars, slots, left, right):
    rows, width = slots.shape
    return pl.pallas_call(
        gather_kernel,
        out_shape=jax.ShapeDtypeStruct((width // LANES, rows, LANES), jnp.bfloat16),
        in_specs=[pl.BlockSpec(memory_space=pltpu.SMEM)]
        + [pl.BlockSpec(memory_space=pltpu.VMEM)] * 3,
        out_specs=pl.BlockSpec(memory_space=pltpu.VMEM),
        cost_estimate=pl.CostEstimate(
            flops=2 * rows * (rows + 2 * EDGE) * width,
            bytes_accessed=4 * rows * width,
            transcendentals=0,
        ),
        compiler_params=SMALL,
        name="gather_rows",
    )(scalars, slots, left, right)


def project_half(side, plane, owned, block):
    planes, _, _ = owned.shape
    deep = (block.shape[1] - 8) // 6
    total = None
    for pair in range(block.shape[0] // 2):
        inputs, weights = [], []
        for kind in range(2):
            north, south = (SHIFTS[kind][4 * pair + c] for c in range(2))
            shard = lax.rem(plane + planes - jnp.where(side == 0, north, south), planes)
            inputs.append(owned[shard])
            at = kind * 3 * deep
            for chip in (2 * pair, 2 * pair + 1):
                weights.append(
                    jnp.concatenate(
                        [block[chip, at + i * deep : at + (i + 1) * deep] for i in range(3)],
                        axis=1,
                    )
                )
        part = jnp.dot(
            jnp.concatenate(inputs, axis=1),
            jnp.concatenate(weights, axis=0),
            preferred_element_type=jnp.float32,
        )
        total = part if total is None else total + part
    return total


def tokens_before(side, index, block):
    last = block.shape[1] - 8
    total = jnp.zeros((8, block.shape[2]), jnp.float32)
    for chip in range(block.shape[0]):
        total += jnp.where(2 * chip + side < index, block[chip, last:].astype(jnp.float32), 0.0)
    return total


def project_kernel(scalars, owned, half, projected, before):
    core, plane, index = (scalars[i] for i in range(2, 5))
    projected[...] = project_half(core, plane, owned, half)
    before[...] = tokens_before(core, index, half)


def project(scalars, owned, half):
    _, rows, lanes = owned.shape
    chips, deep, width = half.shape[0], (half.shape[1] - 8) // 6, 3 * lanes
    return pl.pallas_call(
        project_kernel,
        out_shape=(
            jax.ShapeDtypeStruct((rows, width), jnp.float32),
            jax.ShapeDtypeStruct((8, lanes), jnp.float32),
        ),
        in_specs=[pl.BlockSpec(memory_space=pltpu.SMEM)]
        + [pl.BlockSpec(memory_space=pltpu.VMEM)] * 2,
        out_specs=(pl.BlockSpec(memory_space=pltpu.VMEM),) * 2,
        compiler_params=SMALL,
        cost_estimate=pl.CostEstimate(
            flops=4 * rows * chips * deep * width, bytes_accessed=0, transcendentals=0
        ),
        name="project",
    )(scalars, owned, half)


def attend_kernel(scalars, owned, projected, before, other, ends, attended):
    rows = owned.shape[1]
    head_dim = attended.shape[1]
    shift, count, core, plane, index = (scalars[i] for i in range(5))
    before = before[...] + tokens_before(1 - core, index, other)
    start = before[:1, :1].astype(jnp.int32) + shift
    projected = (projected[...] + project_half(1 - core, plane, owned, other)).astype(
        jnp.bfloat16
    )
    query, keys, values = (projected[:, i * head_dim : (i + 1) * head_dim] for i in range(3))
    scores = lax.dot_general(
        query, keys, (((1,), (1,)), ((), ())), preferred_element_type=jnp.float32
    ) / math.sqrt(head_dim)
    row = lax.broadcasted_iota(jnp.int32, (rows, 1), 0)
    key = lax.broadcasted_iota(jnp.int32, (rows, rows), 1)
    passed = jnp.where(ends[...] <= row + start, ends[...], 0)
    opened = jnp.max(passed, axis=1, keepdims=True) - start
    live = row < count
    allowed = (key <= row) & (key >= opened) & live
    masked = jnp.where(allowed, scores, -1e30)
    peak = jnp.max(masked, axis=1, keepdims=True)
    exponent = jnp.where(allowed, jnp.exp(masked - peak), 0.0)
    denominator = jnp.sum(exponent, axis=1, keepdims=True)
    probs = (exponent / jnp.where(live, denominator, 1.0)).astype(jnp.bfloat16)
    result = jnp.dot(probs, values, preferred_element_type=jnp.float32)
    attended[...] = jnp.where(live, result, 0.0).astype(jnp.bfloat16)


def attend(scalars, owned, projected, before, other, ends):
    return pl.pallas_call(
        attend_kernel,
        out_shape=jax.ShapeDtypeStruct(owned.shape[1:], jnp.bfloat16),
        in_specs=[pl.BlockSpec(memory_space=pltpu.SMEM)]
        + [pl.BlockSpec(memory_space=pltpu.VMEM)] * 5,
        out_specs=pl.BlockSpec(memory_space=pltpu.VMEM),
        compiler_params=SMALL,
        name="attend",
    )(scalars, owned, projected, before, other, ends)


def for_each(value, count):
    return jnp.broadcast_to(value[None], (count, *value.shape))


def moved(value, kind):
    planes = lax.axis_size("z")
    pairs = [
        (j * planes + z, j * planes + (z + shift) % planes)
        for j, shift in enumerate(SHIFTS[kind])
        for z in range(planes)
    ]
    return lax.ppermute(value, (*PLANE, "z"), pairs)


def shards(hidden, pad_counts, doc_lengths, range_shift, qkv_weight):
    slots = hidden[0]
    rows = slots.shape[0]
    size, index = lax.axis_size(PLANE), lax.axis_index(PLANE)
    padding = pad_counts[0, 0]
    live = rows - padding

    deep = qkv_weight.shape[0] // 2
    own = lax.dynamic_slice_in_dim(qkv_weight, lax.axis_index("x") % 2 * deep, deep, 0)
    own = jnp.concatenate(jnp.split(own, 3, axis=1), axis=0)
    far = moved(own, 1)
    head = lax.dynamic_slice_in_dim(slots, padding, EDGE, 0)
    tail = slots[rows - EDGE :]
    left = lax.ppermute(tail, PLANE, [(i, i + 1) for i in range(size - 1)])
    right = lax.ppermute(head, PLANE, [(i + 1, i) for i in range(size - 1)])
    near = moved(own, 0)

    chips = lax.axis_size(("y", "x"))
    tally = jnp.full((8, own.shape[1]), live).astype(jnp.bfloat16)
    half = lax.all_to_all(
        for_each(jnp.concatenate([near, far, tally]), chips), ("y", "x"), 0, 0, tiled=True
    )
    shifts = range_shift[0]
    shift = jnp.where(index == 0, 0, shifts[index])
    following = jnp.where(index == size - 1, 0, shifts[jnp.minimum(index + 1, size - 1)])
    count = live + following - shift
    scalars = jnp.stack([padding, live, shift, count]).astype(jnp.int32)
    owned = gather_rows(scalars, slots, left, right)
    ends = jnp.cumsum(doc_lengths[0])[None]
    where = jnp.stack(
        [shift, count, lax.axis_index("core"), lax.axis_index("z"), index]
    ).astype(jnp.int32)
    half, owned, ends, where = lax.optimization_barrier((half, owned, ends, where))

    other = lax.ppermute(half, "core", [(0, 1), (1, 0)])
    projected, before = project(where, owned, half)
    return attend(where, owned, projected, before, other, ends)[None]


def solution(mesh):
    fine = Mesh(mesh.devices.reshape(4, 4, 2, -1), ("y", "x", "core", "z"))
    in_specs = (P("z", PLANE, None), P("z", PLANE), P("z", None), P("z", None), P("z", None))
    return jax.shard_map(
        shards, mesh=fine, in_specs=in_specs, out_specs=P("z", PLANE, None), check_vma=False
    )
```

```python
import math

import jax
import jax.numpy as jnp
from jax import lax
from jax.experimental import pallas as pl
from jax.experimental.pallas import tpu as pltpu
from jax.sharding import Mesh
from jax.sharding import PartitionSpec as P

PLANE = ("y", "x", "core")
EDGE = 32
SIDE = 4
NEAR = [d for k in range(8) for _ in range(2) for d in ((k, -k) if k else (0, 8))]
FAR = [d for k in range(8) for _ in range(2) for d in ((16 - k, k - 16) if k else (16, -8))]
SHIFTS = (NEAR, FAR)
SMALL = pltpu.CompilerParams(vmem_limit_bytes=16 * 1024 * 1024)


def project_half(side, plane, sources, block):
    lanes = block.shape[2]
    planes = sources[0].shape[1] // lanes
    deep = (block.shape[1] - 8) // 6
    total = None
    for pair in range(block.shape[0] // 2):
        inputs, weights = [], []
        for kind in range(2):
            north, south = (SHIFTS[kind][4 * pair + c] for c in range(2))
            shard = lax.rem(plane + planes - jnp.where(side == 0, north, south), planes)
            columns = pl.ds(pl.multiple_of(shard * lanes, lanes), lanes)
            inputs.append(jnp.concatenate([rows[:, columns] for rows in sources], axis=0))
            at = kind * 3 * deep
            for chip in (2 * pair, 2 * pair + 1):
                weights.append(
                    jnp.concatenate(
                        [block[chip, at + i * deep : at + (i + 1) * deep] for i in range(3)],
                        axis=1,
                    )
                )
        part = jnp.dot(
            jnp.concatenate(inputs, axis=1),
            jnp.concatenate(weights, axis=0),
            preferred_element_type=jnp.float32,
        )
        total = part if total is None else total + part
    return total


def tokens_before(side, index, block):
    last = block.shape[1] - 8
    total = jnp.zeros((8, block.shape[2]), jnp.float32)
    for chip in range(block.shape[0]):
        owner = jnp.where(side == 0, device(chip, 0), device(chip, 1))
        total += jnp.where(owner < index, block[chip, last:].astype(jnp.float32), 0.0)
    return total


def project_kernel(scalars, slots, left, right, half, projected, before):
    side, plane, index = (scalars[i] for i in range(4, 7))
    projected[...] = project_half(side, plane, (slots, left, right), half)
    before[...] = tokens_before(side, index, half)


def project(scalars, slots, left, right, half):
    rows = slots.shape[0] + left.shape[0] + right.shape[0]
    chips, deep, lanes = half.shape[0], (half.shape[1] - 8) // 6, half.shape[2]
    return pl.pallas_call(
        project_kernel,
        out_shape=(
            jax.ShapeDtypeStruct((rows, 3 * lanes), jnp.float32),
            jax.ShapeDtypeStruct((8, lanes), jnp.float32),
        ),
        in_specs=[pl.BlockSpec(memory_space=pltpu.SMEM)]
        + [pl.BlockSpec(memory_space=pltpu.VMEM)] * 4,
        out_specs=(pl.BlockSpec(memory_space=pltpu.VMEM),) * 2,
        compiler_params=SMALL,
        cost_estimate=pl.CostEstimate(
            flops=12 * rows * chips * deep * lanes, bytes_accessed=0, transcendentals=0
        ),
        name="project",
    )(scalars, slots, left, right, half)


def attend_kernel(
    scalars, slots, left, right, projected, before, other, ends, attended
):
    rows, head_dim = attended.shape
    padding, held, shift, count, side, plane, index = (scalars[i] for i in range(7))
    before = before[...] + tokens_before(1 - side, index, other)
    start = before[:1, :1].astype(jnp.int32) + shift
    sources = (slots, left, right)
    projected = (projected[...] + project_half(1 - side, plane, sources, other)).astype(
        jnp.bfloat16
    )
    row = lax.broadcasted_iota(jnp.int32, (rows, 1), 0)
    live = row < count
    offset = row + shift
    source = jnp.where(
        offset < 0,
        rows + EDGE + offset,
        jnp.where(offset < held, padding + offset, rows + EDGE + offset - held),
    )
    source = jnp.where(live, source, -1)
    columns = lax.broadcasted_iota(jnp.int32, (rows, projected.shape[0]), 1)
    picked = jnp.where(columns == source, 1.0, 0.0).astype(jnp.bfloat16)
    projected = jnp.dot(picked, projected, preferred_element_type=jnp.float32).astype(
        jnp.bfloat16
    )
    query, keys, values = (projected[:, i * head_dim : (i + 1) * head_dim] for i in range(3))
    scores = lax.dot_general(
        query, keys, (((1,), (1,)), ((), ())), preferred_element_type=jnp.float32
    ) / math.sqrt(head_dim)
    key = lax.broadcasted_iota(jnp.int32, (rows, rows), 1)
    passed = jnp.where(ends[...] <= row + start, ends[...], 0)
    opened = jnp.max(passed, axis=1, keepdims=True) - start
    allowed = (key <= row) & (key >= opened) & live
    masked = jnp.where(allowed, scores, -1e30)
    peak = jnp.max(masked, axis=1, keepdims=True)
    exponent = jnp.where(allowed, jnp.exp(masked - peak), 0.0)
    denominator = jnp.sum(exponent, axis=1, keepdims=True)
    probs = (exponent / jnp.where(live, denominator, 1.0)).astype(jnp.bfloat16)
    result = jnp.dot(probs, values, preferred_element_type=jnp.float32)
    attended[...] = jnp.where(live, result, 0.0).astype(jnp.bfloat16)


def attend(scalars, slots, left, right, projected, before, other, ends):
    return pl.pallas_call(
        attend_kernel,
        out_shape=jax.ShapeDtypeStruct((slots.shape[0], other.shape[2]), jnp.bfloat16),
        in_specs=[pl.BlockSpec(memory_space=pltpu.SMEM)]
        + [pl.BlockSpec(memory_space=pltpu.VMEM)] * 7,
        out_specs=pl.BlockSpec(memory_space=pltpu.VMEM),
        compiler_params=SMALL,
        name="attend",
    )(scalars, slots, left, right, projected, before, other, ends)


def for_each(value, count):
    return jnp.broadcast_to(value[None], (count, *value.shape))


def device(place, side):
    chip = place if side == 0 else place % SIDE * SIDE + place // SIDE
    return 2 * chip + (side + chip % SIDE + chip // SIDE) % 2


def moved(value, kind):
    planes = lax.axis_size("z")
    pairs = [
        (device(place, side) * planes + z, device(place, side) * planes + (z + shift) % planes)
        for place in range(SIDE * SIDE)
        for side, shift in enumerate(SHIFTS[kind][2 * place : 2 * place + 2])
        for z in range(planes)
    ]
    return lax.ppermute(value, (*PLANE, "z"), pairs)


def spread(value, step):
    lines = [[SIDE * i + at for at in range(SIDE)] for i in range(SIDE)]
    if step:
        lines = [list(line) for line in zip(*lines)]
    groups = [[device(place, side) for place in line] for line in lines for side in range(2)]
    return lax.all_to_all(
        for_each(value, SIDE), PLANE, 0, 0, axis_index_groups=groups, tiled=True
    )


def shards(hidden, pad_counts, doc_lengths, range_shift, qkv_weight):
    slots = hidden[0]
    rows = slots.shape[0]
    size, index = lax.axis_size(PLANE), lax.axis_index(PLANE)
    padding = pad_counts[0, 0]
    live = rows - padding

    deep = qkv_weight.shape[0] // 2
    x, y = lax.axis_index("x"), lax.axis_index("y")
    side = (lax.axis_index("core") + x + y) % 2
    upper = jnp.where(side == 0, x, y) % 2
    own = lax.dynamic_slice_in_dim(qkv_weight, upper * deep, deep, 0)
    own = jnp.concatenate(jnp.split(own, 3, axis=1), axis=0)
    far = moved(own, 1)
    head = lax.dynamic_slice_in_dim(slots, padding, EDGE, 0)
    tail = slots[rows - EDGE :]
    left = lax.ppermute(tail, PLANE, [(i, i + 1) for i in range(size - 1)])
    right = lax.ppermute(head, PLANE, [(i + 1, i) for i in range(size - 1)])
    near = moved(own, 0)

    shifts = range_shift[0]
    shift = jnp.where(index == 0, 0, shifts[index])
    following = jnp.where(index == size - 1, 0, shifts[jnp.minimum(index + 1, size - 1)])
    count = live + following - shift
    ends = jnp.cumsum(doc_lengths[0])[None]
    scalars = jnp.stack(
        [padding, live, shift, count, side, lax.axis_index("z"), index]
    ).astype(jnp.int32)
    near, far, ends, scalars = lax.optimization_barrier((near, far, ends, scalars))
    tally = jnp.full((8, own.shape[1]), live).astype(jnp.bfloat16)
    line = spread(jnp.concatenate([near, far, tally]), 0)
    half = spread(line, 1).reshape(-1, *line.shape[1:])
    other = lax.ppermute(half, "core", [(0, 1), (1, 0)])
    projected, before = project(scalars, slots, left, right, half)
    return attend(scalars, slots, left, right, projected, before, other, ends)[None]


def solution(mesh):
    fine = Mesh(mesh.devices.reshape(4, 4, 2, -1), ("y", "x", "core", "z"))
    in_specs = (P("z", PLANE, None), P("z", PLANE), P("z", None), P("z", None), P("z", None))
    return jax.shard_map(
        shards, mesh=fine, in_specs=in_specs, out_specs=P("z", PLANE, None), check_vma=False
    )
```

```python
import math

import jax
import jax.numpy as jnp
from jax import lax
from jax.experimental import pallas as pl
from jax.experimental.pallas import tpu as pltpu
from jax.sharding import Mesh
from jax.sharding import PartitionSpec as P

PLANE = ("y", "x", "core")
EDGE = 32
SIDE = 4
STEPS = (0, 1, 3, 2)
NEAR = [d for k in range(8) for _ in range(2) for d in ((k, -k) if k else (0, 8))]
FAR = [d for k in range(8) for _ in range(2) for d in ((16 - k, k - 16) if k else (16, -8))]
SHIFTS = (NEAR, FAR)
SMALL = pltpu.CompilerParams(vmem_limit_bytes=16 * 1024 * 1024)


def distance(k, side, kind):
    if kind == 0:
        return jnp.where(side == 0, k, jnp.where(k == 0, 8, -k))
    return jnp.where(side == 0, 16 - k, jnp.where(k == 0, -8, k - 16))


def project_half(side, at, plane, sources, blocks):
    lanes = blocks[0].shape[2]
    planes = sources[0].shape[1] // lanes
    deep = (blocks[0].shape[1] - 8) // 6
    total = None
    for step, block in zip(STEPS, blocks):
        line = lax.rem(at + SIDE - step, SIDE)
        for pair in range(SIDE // 2):
            inputs, weights = [], []
            for kind in range(2):
                shift = distance(SIDE // 2 * line + pair, side, kind)
                shard = lax.rem(plane + planes - shift, planes)
                columns = pl.ds(pl.multiple_of(shard * lanes, lanes), lanes)
                inputs.append(jnp.concatenate([rows[:, columns] for rows in sources], axis=0))
                first = kind * 3 * deep
                for place in (2 * pair, 2 * pair + 1):
                    weights.append(
                        jnp.concatenate(
                            [
                                block[place, first + i * deep : first + (i + 1) * deep]
                                for i in range(3)
                            ],
                            axis=1,
                        )
                    )
            part = jnp.dot(
                jnp.concatenate(inputs, axis=1),
                jnp.concatenate(weights, axis=0),
                preferred_element_type=jnp.float32,
            )
            total = part if total is None else total + part
    return total


def tokens_before(side, at, index, blocks):
    last = blocks[0].shape[1] - 8
    total = jnp.zeros((8, blocks[0].shape[2]), jnp.float32)
    for step, block in zip(STEPS, blocks):
        line = lax.rem(at + SIDE - step, SIDE)
        for place in range(SIDE):
            chip = jnp.where(side == 0, SIDE * line + place, SIDE * place + line)
            owner = 2 * chip + lax.rem(side + line + place, 2)
            total += jnp.where(owner < index, block[place, last:].astype(jnp.float32), 0.0)
    return total


def project_kernel(scalars, slots, left, right, *rest):
    blocks, (projected, before) = rest[:SIDE], rest[SIDE:]
    side, at, plane, index = (scalars[i] for i in (4, 5, 7, 8))
    projected[...] = project_half(side, at, plane, (slots, left, right), blocks)
    before[...] = tokens_before(side, at, index, blocks)


def project(scalars, slots, left, right, blocks):
    rows = slots.shape[0] + left.shape[0] + right.shape[0]
    lanes = blocks[0].shape[2]
    return pl.pallas_call(
        project_kernel,
        out_shape=(
            jax.ShapeDtypeStruct((rows, 3 * lanes), jnp.float32),
            jax.ShapeDtypeStruct((8, lanes), jnp.float32),
        ),
        in_specs=[pl.BlockSpec(memory_space=pltpu.SMEM)]
        + [pl.BlockSpec(memory_space=pltpu.VMEM)] * (3 + SIDE),
        out_specs=(pl.BlockSpec(memory_space=pltpu.VMEM),) * 2,
        compiler_params=SMALL,
        cost_estimate=pl.CostEstimate(
            flops=3 * rows * slots.shape[1] * lanes, bytes_accessed=0, transcendentals=0
        ),
        name="project",
    )(scalars, slots, left, right, *blocks)


def attend_kernel(scalars, slots, left, right, projected, before, ends, *rest):
    blocks, attended = rest[:SIDE], rest[SIDE]
    rows, head_dim = attended.shape
    padding, held, shift, count, side, _, at, plane, index = (scalars[i] for i in range(9))
    before = before[...] + tokens_before(1 - side, at, index, blocks)
    start = before[:1, :1].astype(jnp.int32) + shift
    sources = (slots, left, right)
    projected = (projected[...] + project_half(1 - side, at, plane, sources, blocks)).astype(
        jnp.bfloat16
    )
    row = lax.broadcasted_iota(jnp.int32, (rows, 1), 0)
    live = row < count
    offset = row + shift
    source = jnp.where(
        offset < 0,
        rows + EDGE + offset,
        jnp.where(offset < held, padding + offset, rows + EDGE + offset - held),
    )
    source = jnp.where(live, source, -1)
    columns = lax.broadcasted_iota(jnp.int32, (rows, projected.shape[0]), 1)
    picked = jnp.where(columns == source, 1.0, 0.0).astype(jnp.bfloat16)
    projected = jnp.dot(picked, projected, preferred_element_type=jnp.float32).astype(
        jnp.bfloat16
    )
    query, keys, values = (projected[:, i * head_dim : (i + 1) * head_dim] for i in range(3))
    scores = lax.dot_general(
        query, keys, (((1,), (1,)), ((), ())), preferred_element_type=jnp.float32
    ) / math.sqrt(head_dim)
    key = lax.broadcasted_iota(jnp.int32, (rows, rows), 1)
    passed = jnp.where(ends[...] <= row + start, ends[...], 0)
    opened = jnp.max(passed, axis=1, keepdims=True) - start
    allowed = (key <= row) & (key >= opened) & live
    masked = jnp.where(allowed, scores, -1e30)
    peak = jnp.max(masked, axis=1, keepdims=True)
    exponent = jnp.where(allowed, jnp.exp(masked - peak), 0.0)
    denominator = jnp.sum(exponent, axis=1, keepdims=True)
    probs = (exponent / jnp.where(live, denominator, 1.0)).astype(jnp.bfloat16)
    result = jnp.dot(probs, values, preferred_element_type=jnp.float32)
    attended[...] = jnp.where(live, result, 0.0).astype(jnp.bfloat16)


def attend(scalars, slots, left, right, projected, before, ends, blocks):
    return pl.pallas_call(
        attend_kernel,
        out_shape=jax.ShapeDtypeStruct((slots.shape[0], ends.shape[1]), jnp.bfloat16),
        in_specs=[pl.BlockSpec(memory_space=pltpu.SMEM)]
        + [pl.BlockSpec(memory_space=pltpu.VMEM)] * (6 + SIDE),
        out_specs=pl.BlockSpec(memory_space=pltpu.VMEM),
        compiler_params=SMALL,
        name="attend",
    )(scalars, slots, left, right, projected, before, ends, *blocks)


def for_each(value, count):
    return jnp.broadcast_to(value[None], (count, *value.shape))


def device(place, side):
    chip = place if side == 0 else place % SIDE * SIDE + place // SIDE
    return 2 * chip + (side + chip % SIDE + chip // SIDE) % 2


def moved(value, kind):
    planes = lax.axis_size("z")
    pairs = [
        (device(place, side) * planes + z, device(place, side) * planes + (z + shift) % planes)
        for place in range(SIDE * SIDE)
        for side, shift in enumerate(SHIFTS[kind][2 * place : 2 * place + 2])
        for z in range(planes)
    ]
    return lax.ppermute(value, (*PLANE, "z"), pairs)


def line_of(value):
    groups = [
        [device(SIDE * at + place, side) for place in range(SIDE)]
        for at in range(SIDE)
        for side in range(2)
    ]
    return lax.all_to_all(
        for_each(value, SIDE), PLANE, 0, 0, axis_index_groups=groups, tiled=True
    )


def passed_on(value, step):
    pairs = [
        (device(place, side), device((place + SIDE * step) % SIDE**2, side))
        for place in range(SIDE**2)
        for side in range(2)
    ]
    return lax.ppermute(value, PLANE, pairs)


def shards(hidden, pad_counts, doc_lengths, range_shift, qkv_weight):
    slots = hidden[0]
    rows = slots.shape[0]
    size, index = lax.axis_size(PLANE), lax.axis_index(PLANE)
    padding = pad_counts[0, 0]
    live = rows - padding

    deep = qkv_weight.shape[0] // 2
    x, y = lax.axis_index("x"), lax.axis_index("y")
    side = (lax.axis_index("core") + x + y) % 2
    upper = jnp.where(side == 0, x, y) % 2
    own = lax.dynamic_slice_in_dim(qkv_weight, upper * deep, deep, 0)
    own = jnp.concatenate(jnp.split(own, 3, axis=1), axis=0)
    far = moved(own, 1)
    head = lax.dynamic_slice_in_dim(slots, padding, EDGE, 0)
    tail = slots[rows - EDGE :]
    left = lax.ppermute(tail, PLANE, [(i, i + 1) for i in range(size - 1)])
    right = lax.ppermute(head, PLANE, [(i + 1, i) for i in range(size - 1)])
    near = moved(own, 0)

    shifts = range_shift[0]
    shift = jnp.where(index == 0, 0, shifts[index])
    following = jnp.where(index == size - 1, 0, shifts[jnp.minimum(index + 1, size - 1)])
    count = live + following - shift
    ends = jnp.cumsum(doc_lengths[0])[None]
    scalars = jnp.stack(
        [
            padding,
            live,
            shift,
            count,
            side,
            jnp.where(side == 0, y, x),
            jnp.where(side == 0, x, y),
            lax.axis_index("z"),
            index,
        ]
    ).astype(jnp.int32)
    tally = jnp.full((8, own.shape[1]), live).astype(jnp.bfloat16)
    blocks = [line_of(jnp.concatenate([near, far, tally]))]
    for step in STEPS[1:]:
        blocks.append(passed_on(blocks[0], step))
    blocks[-1], ends, scalars = lax.optimization_barrier((blocks[-1], ends, scalars))
    others = []
    for step, block in zip(STEPS, blocks):
        others.append(lax.ppermute(block, "core", [(0, 1), (1, 0)]))
    projected, before = project(scalars, slots, left, right, blocks)
    return attend(scalars, slots, left, right, projected, before, ends, others)[None]


def solution(mesh):
    fine = Mesh(mesh.devices.reshape(4, 4, 2, -1), ("y", "x", "core", "z"))
    in_specs = (P("z", PLANE, None), P("z", PLANE), P("z", None), P("z", None), P("z", None))
    return jax.shard_map(
        shards, mesh=fine, in_specs=in_specs, out_specs=P("z", PLANE, None), check_vma=False
    )
```

```python
import math

import jax
import jax.numpy as jnp
from jax import lax
from jax.experimental import pallas as pl
from jax.experimental.pallas import tpu as pltpu
from jax.sharding import Mesh
from jax.sharding import PartitionSpec as P

PLANE = ("y", "x", "core")
EDGE = 32
SIDE = 4
STEPS = (0, 1, 3, 2)
NEAR = [d for k in range(8) for _ in range(2) for d in ((k, -k) if k else (0, 8))]
FAR = [d for k in range(8) for _ in range(2) for d in ((16 - k, k - 16) if k else (16, -8))]
SHIFTS = (NEAR, FAR)
SMALL = pltpu.CompilerParams(vmem_limit_bytes=16 * 1024 * 1024)


def distance(k, side, kind):
    if kind == 0:
        return jnp.where(side == 0, k, jnp.where(k == 0, 8, -k))
    return jnp.where(side == 0, 16 - k, jnp.where(k == 0, -8, k - 16))


def project_half(side, at, plane, sources, blocks):
    lanes = blocks[0].shape[2]
    planes = sources[0].shape[1] // lanes
    deep = (blocks[0].shape[1] - 8) // 6
    total = None
    for step, block in zip(STEPS, blocks):
        line = lax.rem(at + SIDE - step, SIDE)
        for pair in range(SIDE // 2):
            inputs, weights = [], []
            for kind in range(2):
                shift = distance(SIDE // 2 * line + pair, side, kind)
                shard = lax.rem(plane + planes - shift, planes)
                columns = pl.ds(pl.multiple_of(shard * lanes, lanes), lanes)
                inputs.append(jnp.concatenate([rows[:, columns] for rows in sources], axis=0))
                first = kind * 3 * deep
                for place in (2 * pair, 2 * pair + 1):
                    weights.append(
                        jnp.concatenate(
                            [
                                block[place, first + i * deep : first + (i + 1) * deep]
                                for i in range(3)
                            ],
                            axis=1,
                        )
                    )
            part = jnp.dot(
                jnp.concatenate(inputs, axis=1),
                jnp.concatenate(weights, axis=0),
                preferred_element_type=jnp.float32,
            )
            total = part if total is None else total + part
    return total


def tokens_before(side, at, index, blocks):
    last = blocks[0].shape[1] - 8
    total = jnp.zeros((8, blocks[0].shape[2]), jnp.float32)
    for step, block in zip(STEPS, blocks):
        line = lax.rem(at + SIDE - step, SIDE)
        for place in range(SIDE):
            chip = jnp.where(side == 0, SIDE * line + place, SIDE * place + line)
            owner = 2 * chip + lax.rem(side + line + place, 2)
            total += jnp.where(owner < index, block[place, last:].astype(jnp.float32), 0.0)
    return total


def parts_of(joined, last):
    return [joined.at[i * SIDE : (i + 1) * SIDE] for i in range(SIDE - 1)] + [last]


def project_kernel(
    scalars, slots, left, right, lengths, joined, last, projected, before, ends
):
    side, at, _, plane, index = (scalars[i] for i in range(5))
    blocks = parts_of(joined, last)
    projected[...] = project_half(side, at, plane, (slots, left, right), blocks)
    before[...] = tokens_before(side, at, index, blocks)
    total = jnp.broadcast_to(lengths[...], ends.shape)
    lane = lax.broadcasted_iota(jnp.int32, ends.shape, 1)
    reach = 1
    while reach < ends.shape[1]:
        total += jnp.where(lane >= reach, pltpu.roll(total, reach, 1), 0)
        reach *= 2
    ends[...] = total


def project(scalars, slots, left, right, lengths, joined, last):
    rows = slots.shape[0] + left.shape[0] + right.shape[0]
    lanes = last.shape[2]
    return pl.pallas_call(
        project_kernel,
        out_shape=(
            jax.ShapeDtypeStruct((rows, 3 * lanes), jnp.float32),
            jax.ShapeDtypeStruct((8, lanes), jnp.float32),
            jax.ShapeDtypeStruct((8, lengths.shape[1]), jnp.int32),
        ),
        in_specs=[pl.BlockSpec(memory_space=pltpu.SMEM)]
        + [pl.BlockSpec(memory_space=pltpu.VMEM)] * 6,
        out_specs=(pl.BlockSpec(memory_space=pltpu.VMEM),) * 3,
        compiler_params=SMALL,
        cost_estimate=pl.CostEstimate(
            flops=3 * rows * slots.shape[1] * lanes, bytes_accessed=0, transcendentals=0
        ),
        name="project",
    )(scalars, slots, left, right, lengths, joined, last)


def attend_kernel(
    scalars, pads, shifts, slots, left, right, projected, before, ends, joined, last, attended
):
    blocks = parts_of(joined, last)
    rows, head_dim = attended.shape
    side, _, at, plane, index = (scalars[i] for i in range(5))
    devices = shifts.shape[1]
    padding = pads[0, 0]
    held = rows - padding
    shift = jnp.where(index == 0, 0, shifts[0, index])
    following = shifts[0, jnp.minimum(index + 1, devices - 1)]
    count = held - shift + jnp.where(index == devices - 1, 0, following)
    before = before[...] + tokens_before(1 - side, at, index, blocks)
    start = before[:1, :1].astype(jnp.int32) + shift
    sources = (slots, left, right)
    projected = (projected[...] + project_half(1 - side, at, plane, sources, blocks)).astype(
        jnp.bfloat16
    )
    row = lax.broadcasted_iota(jnp.int32, (rows, 1), 0)
    live = row < count
    offset = row + shift
    source = jnp.where(
        offset < 0,
        rows + EDGE + offset,
        jnp.where(offset < held, padding + offset, rows + EDGE + offset - held),
    )
    source = jnp.where(live, source, -1)
    columns = lax.broadcasted_iota(jnp.int32, (rows, projected.shape[0]), 1)
    picked = jnp.where(columns == source, 1.0, 0.0).astype(jnp.bfloat16)
    projected = jnp.dot(picked, projected, preferred_element_type=jnp.float32).astype(
        jnp.bfloat16
    )
    query, keys, values = (projected[:, i * head_dim : (i + 1) * head_dim] for i in range(3))
    scores = lax.dot_general(
        query, keys, (((1,), (1,)), ((), ())), preferred_element_type=jnp.float32
    ) / math.sqrt(head_dim)
    key = lax.broadcasted_iota(jnp.int32, (rows, rows), 1)
    passed = jnp.where(ends[:1] <= row + start, ends[:1], 0)
    opened = jnp.max(passed, axis=1, keepdims=True) - start
    allowed = (key <= row) & (key >= opened) & live
    masked = jnp.where(allowed, scores, -1e30)
    peak = jnp.max(masked, axis=1, keepdims=True)
    exponent = jnp.where(allowed, jnp.exp(masked - peak), 0.0)
    denominator = jnp.sum(exponent, axis=1, keepdims=True)
    probs = (exponent / jnp.where(live, denominator, 1.0)).astype(jnp.bfloat16)
    result = jnp.dot(probs, values, preferred_element_type=jnp.float32)
    attended[...] = jnp.where(live, result, 0.0).astype(jnp.bfloat16)


def attend(scalars, pads, shifts, slots, left, right, projected, before, ends, joined, last):
    return pl.pallas_call(
        attend_kernel,
        out_shape=jax.ShapeDtypeStruct((slots.shape[0], last.shape[2]), jnp.bfloat16),
        in_specs=[pl.BlockSpec(memory_space=pltpu.SMEM)] * 3
        + [pl.BlockSpec(memory_space=pltpu.VMEM)] * 8,
        out_specs=pl.BlockSpec(memory_space=pltpu.VMEM),
        compiler_params=SMALL,
        name="attend",
    )(scalars, pads, shifts, slots, left, right, projected, before, ends, joined, last)


def join_kernel(*refs):
    places = refs[0].shape[0]
    for at, block in enumerate(refs[:-1]):
        refs[-1][at * places : (at + 1) * places] = block[...]


def join(blocks):
    places, deep, lanes = blocks[0].shape
    return pl.pallas_call(
        join_kernel,
        out_shape=jax.ShapeDtypeStruct((len(blocks) * places, deep, lanes), jnp.bfloat16),
        in_specs=[pl.BlockSpec(memory_space=pltpu.VMEM)] * len(blocks),
        out_specs=pl.BlockSpec(memory_space=pltpu.VMEM),
        compiler_params=SMALL,
        name="join",
    )(*blocks)


def for_each(value, count):
    return jnp.broadcast_to(value[None], (count, *value.shape))


def device(place, side):
    chip = place if side == 0 else place % SIDE * SIDE + place // SIDE
    return 2 * chip + (side + chip % SIDE + chip // SIDE) % 2


def moved(value, kind):
    planes = lax.axis_size("z")
    pairs = [
        (device(place, side) * planes + z, device(place, side) * planes + (z + shift) % planes)
        for place in range(SIDE * SIDE)
        for side, shift in enumerate(SHIFTS[kind][2 * place : 2 * place + 2])
        for z in range(planes)
    ]
    return lax.ppermute(value, (*PLANE, "z"), pairs)


def line_of(value):
    groups = [
        [device(SIDE * at + place, side) for place in range(SIDE)]
        for at in range(SIDE)
        for side in range(2)
    ]
    return lax.all_to_all(
        for_each(value, SIDE), PLANE, 0, 0, axis_index_groups=groups, tiled=True
    )


def passed_on(value, step):
    pairs = [
        (device(place, side), device((place + SIDE * step) % SIDE**2, side))
        for place in range(SIDE**2)
        for side in range(2)
    ]
    return lax.ppermute(value, PLANE, pairs)


def shards(hidden, pad_counts, doc_lengths, range_shift, qkv_weight):
    slots = hidden[0]
    rows = slots.shape[0]
    size, index = lax.axis_size(PLANE), lax.axis_index(PLANE)
    padding = pad_counts[0, 0]
    live = rows - padding

    deep = qkv_weight.shape[0] // 2
    x, y = lax.axis_index("x"), lax.axis_index("y")
    side = (lax.axis_index("core") + x + y) % 2
    upper = jnp.where(side == 0, x, y) % 2
    own = lax.dynamic_slice_in_dim(qkv_weight, upper * deep, deep, 0)
    own = jnp.concatenate(jnp.split(own, 3, axis=1), axis=0)
    far = moved(own, 1)
    head = lax.dynamic_slice_in_dim(slots, padding, EDGE, 0)
    tail = slots[rows - EDGE :]
    left = lax.ppermute(tail, PLANE, [(i, i + 1) for i in range(size - 1)])
    right = lax.ppermute(head, PLANE, [(i + 1, i) for i in range(size - 1)])
    near = moved(own, 0)

    scalars = jnp.stack(
        [
            side,
            jnp.where(side == 0, y, x),
            jnp.where(side == 0, x, y),
            lax.axis_index("z"),
            index,
        ]
    ).astype(jnp.int32)
    near, far, scalars = lax.optimization_barrier((near, far, scalars))
    tally = jnp.full((8, own.shape[1]), live).astype(jnp.bfloat16)
    line = line_of(jnp.concatenate([near, far, tally]))
    after = passed_on(line, 1)
    ahead = passed_on(line, 3)
    lower = passed_on(after[: SIDE // 2], 1)
    higher = passed_on(ahead[SIDE // 2 :], 3)
    joined, last = join([line, after, ahead]), join([lower, higher])
    mates = [(0, 1), (1, 0)]
    other_joined = lax.ppermute(joined, "core", mates)
    other_last = lax.ppermute(last, "core", mates)
    projected, before, ends = project(
        scalars, slots, left, right, doc_lengths, joined, last
    )
    return attend(
        scalars,
        pad_counts,
        range_shift,
        slots,
        left,
        right,
        projected,
        before,
        ends,
        other_joined,
        other_last,
    )[None]


def solution(mesh):
    fine = Mesh(mesh.devices.reshape(4, 4, 2, -1), ("y", "x", "core", "z"))
    in_specs = (P("z", PLANE, None), P("z", PLANE), P("z", None), P("z", None), P("z", None))
    return jax.shard_map(
        shards, mesh=fine, in_specs=in_specs, out_specs=P("z", PLANE, None), check_vma=False
    )
```

```python
import math

import jax
import jax.numpy as jnp
from jax import lax
from jax.experimental import pallas as pl
from jax.experimental.pallas import tpu as pltpu
from jax.sharding import Mesh
from jax.sharding import PartitionSpec as P

PLANE = ("y", "x", "core")
EDGE = 32
SIDE = 4
STEPS = (0, 1, 3, 2)
NEAR = [d for k in range(8) for _ in range(2) for d in ((k, -k) if k else (0, 8))]
FAR = [d for k in range(8) for _ in range(2) for d in ((16 - k, k - 16) if k else (16, -8))]
SHIFTS = (NEAR, FAR)
SMALL = pltpu.CompilerParams(vmem_limit_bytes=16 * 1024 * 1024)


def distance(k, side, kind):
    if kind == 0:
        return jnp.where(side == 0, k, jnp.where(k == 0, 8, -k))
    return jnp.where(side == 0, 16 - k, jnp.where(k == 0, -8, k - 16))


def project_half(side, at, plane, sources, blocks):
    lanes = blocks[0].shape[2]
    planes = sources[0].shape[1] // lanes
    deep = (blocks[0].shape[1] - 8) // 6
    total = None
    for step, block in zip(STEPS, blocks):
        line = lax.rem(at + SIDE - step, SIDE)
        for pair in range(SIDE // 2):
            inputs, weights = [], []
            for kind in range(2):
                shift = distance(SIDE // 2 * line + pair, side, kind)
                shard = lax.rem(plane + planes - shift, planes)
                columns = pl.ds(pl.multiple_of(shard * lanes, lanes), lanes)
                inputs.append(jnp.concatenate([rows[:, columns] for rows in sources], axis=0))
                first = kind * 3 * deep
                for place in (2 * pair, 2 * pair + 1):
                    weights.append(
                        jnp.concatenate(
                            [
                                block[place, first + i * deep : first + (i + 1) * deep]
                                for i in range(3)
                            ],
                            axis=1,
                        )
                    )
            part = jnp.dot(
                jnp.concatenate(inputs, axis=1),
                jnp.concatenate(weights, axis=0),
                preferred_element_type=jnp.float32,
            )
            total = part if total is None else total + part
    return total


def tokens_before(side, at, index, blocks):
    last = blocks[0].shape[1] - 8
    total = jnp.zeros((8, blocks[0].shape[2]), jnp.float32)
    for step, block in zip(STEPS, blocks):
        line = lax.rem(at + SIDE - step, SIDE)
        for place in range(SIDE):
            chip = jnp.where(side == 0, SIDE * line + place, SIDE * place + line)
            owner = 2 * chip + lax.rem(side + line + place, 2)
            total += jnp.where(owner < index, block[place, last:].astype(jnp.float32), 0.0)
    return total


def parts_of(joined, last):
    return [pair.at[i * SIDE : (i + 1) * SIDE] for pair in (joined, last) for i in range(2)]


def project_kernel(
    scalars, slots, left, right, lengths, joined, last, projected, before, ends
):
    side, at, _, plane, index = (scalars[i] for i in range(5))
    blocks = parts_of(joined, last)
    projected[...] = project_half(side, at, plane, (slots, left, right), blocks)
    before[...] = tokens_before(side, at, index, blocks)
    total = jnp.broadcast_to(lengths[...], ends.shape)
    lane = lax.broadcasted_iota(jnp.int32, ends.shape, 1)
    reach = 1
    while reach < ends.shape[1]:
        total += jnp.where(lane >= reach, pltpu.roll(total, reach, 1), 0)
        reach *= 2
    ends[...] = total


def project(scalars, slots, left, right, lengths, joined, last):
    rows = slots.shape[0] + left.shape[0] + right.shape[0]
    lanes = last.shape[2]
    return pl.pallas_call(
        project_kernel,
        out_shape=(
            jax.ShapeDtypeStruct((rows, 3 * lanes), jnp.float32),
            jax.ShapeDtypeStruct((8, lanes), jnp.float32),
            jax.ShapeDtypeStruct((8, lengths.shape[1]), jnp.int32),
        ),
        in_specs=[pl.BlockSpec(memory_space=pltpu.SMEM)]
        + [pl.BlockSpec(memory_space=pltpu.VMEM)] * 6,
        out_specs=(pl.BlockSpec(memory_space=pltpu.VMEM),) * 3,
        compiler_params=SMALL,
        cost_estimate=pl.CostEstimate(
            flops=3 * rows * slots.shape[1] * lanes, bytes_accessed=0, transcendentals=0
        ),
        name="project",
    )(scalars, slots, left, right, lengths, joined, last)


def attend_kernel(
    scalars, pads, shifts, slots, left, right, projected, before, ends, joined, last, attended
):
    blocks = parts_of(joined, last)
    rows, head_dim = attended.shape
    side, _, at, plane, index = (scalars[i] for i in range(5))
    devices = shifts.shape[1]
    padding = pads[0, 0]
    held = rows - padding
    shift = jnp.where(index == 0, 0, shifts[0, index])
    following = shifts[0, jnp.minimum(index + 1, devices - 1)]
    count = held - shift + jnp.where(index == devices - 1, 0, following)
    before = before[...] + tokens_before(1 - side, at, index, blocks)
    start = before[:1, :1].astype(jnp.int32) + shift
    sources = (slots, left, right)
    projected = (projected[...] + project_half(1 - side, at, plane, sources, blocks)).astype(
        jnp.bfloat16
    )
    row = lax.broadcasted_iota(jnp.int32, (rows, 1), 0)
    live = row < count
    offset = row + shift
    source = jnp.where(
        offset < 0,
        rows + EDGE + offset,
        jnp.where(offset < held, padding + offset, rows + EDGE + offset - held),
    )
    source = jnp.where(live, source, -1)
    columns = lax.broadcasted_iota(jnp.int32, (rows, projected.shape[0]), 1)
    picked = jnp.where(columns == source, 1.0, 0.0).astype(jnp.bfloat16)
    projected = jnp.dot(picked, projected, preferred_element_type=jnp.float32).astype(
        jnp.bfloat16
    )
    query, keys, values = (projected[:, i * head_dim : (i + 1) * head_dim] for i in range(3))
    scores = lax.dot_general(
        query, keys, (((1,), (1,)), ((), ())), preferred_element_type=jnp.float32
    ) / math.sqrt(head_dim)
    key = lax.broadcasted_iota(jnp.int32, (rows, rows), 1)
    passed = jnp.where(ends[:1] <= row + start, ends[:1], 0)
    opened = jnp.max(passed, axis=1, keepdims=True) - start
    allowed = (key <= row) & (key >= opened) & live
    masked = jnp.where(allowed, scores, -1e30)
    peak = jnp.max(masked, axis=1, keepdims=True)
    exponent = jnp.where(allowed, jnp.exp(masked - peak), 0.0)
    denominator = jnp.sum(exponent, axis=1, keepdims=True)
    probs = (exponent / jnp.where(live, denominator, 1.0)).astype(jnp.bfloat16)
    result = jnp.dot(probs, values, preferred_element_type=jnp.float32)
    attended[...] = jnp.where(live, result, 0.0).astype(jnp.bfloat16)


def attend(scalars, pads, shifts, slots, left, right, projected, before, ends, joined, last):
    return pl.pallas_call(
        attend_kernel,
        out_shape=jax.ShapeDtypeStruct((slots.shape[0], last.shape[2]), jnp.bfloat16),
        in_specs=[pl.BlockSpec(memory_space=pltpu.SMEM)] * 3
        + [pl.BlockSpec(memory_space=pltpu.VMEM)] * 8,
        out_specs=pl.BlockSpec(memory_space=pltpu.VMEM),
        compiler_params=SMALL,
        name="attend",
    )(scalars, pads, shifts, slots, left, right, projected, before, ends, joined, last)


def join_kernel(*refs):
    for at, block in enumerate(refs[:-1]):
        refs[-1][at * SIDE : (at + 1) * SIDE] = block[...]


def join(blocks):
    places, deep, lanes = blocks[0].shape
    return pl.pallas_call(
        join_kernel,
        out_shape=jax.ShapeDtypeStruct((len(blocks) * places, deep, lanes), jnp.bfloat16),
        in_specs=[pl.BlockSpec(memory_space=pltpu.VMEM)] * len(blocks),
        out_specs=pl.BlockSpec(memory_space=pltpu.VMEM),
        compiler_params=SMALL,
        name="join",
    )(*blocks)


def for_each(value, count):
    return jnp.broadcast_to(value[None], (count, *value.shape))


def device(place, side):
    chip = place if side == 0 else place % SIDE * SIDE + place // SIDE
    return 2 * chip + (side + chip % SIDE + chip // SIDE) % 2


def moved(value, kind):
    planes = lax.axis_size("z")
    pairs = [
        (device(place, side) * planes + z, device(place, side) * planes + (z + shift) % planes)
        for place in range(SIDE * SIDE)
        for side, shift in enumerate(SHIFTS[kind][2 * place : 2 * place + 2])
        for z in range(planes)
    ]
    return lax.ppermute(value, (*PLANE, "z"), pairs)


def line_of(value):
    groups = [
        [device(SIDE * at + place, side) for place in range(SIDE)]
        for at in range(SIDE)
        for side in range(2)
    ]
    return lax.all_to_all(
        for_each(value, SIDE), PLANE, 0, 0, axis_index_groups=groups, tiled=True
    )


def passed_on(value, step):
    pairs = [
        (device(place, side), device((place + SIDE * step) % SIDE**2, side))
        for place in range(SIDE**2)
        for side in range(2)
    ]
    return lax.ppermute(value, PLANE, pairs)


def shards(hidden, pad_counts, doc_lengths, range_shift, qkv_weight):
    slots = hidden[0]
    rows = slots.shape[0]
    size, index = lax.axis_size(PLANE), lax.axis_index(PLANE)
    padding = pad_counts[0, 0]
    live = rows - padding

    deep = qkv_weight.shape[0] // 2
    x, y = lax.axis_index("x"), lax.axis_index("y")
    side = (lax.axis_index("core") + x + y) % 2
    upper = jnp.where(side == 0, x, y) % 2
    own = lax.dynamic_slice_in_dim(qkv_weight, upper * deep, deep, 0)
    own = jnp.concatenate(jnp.split(own, 3, axis=1), axis=0)
    far = moved(own, 1)
    head = lax.dynamic_slice_in_dim(slots, padding, EDGE, 0)
    tail = slots[rows - EDGE :]
    left = lax.ppermute(tail, PLANE, [(i, i + 1) for i in range(size - 1)])
    right = lax.ppermute(head, PLANE, [(i + 1, i) for i in range(size - 1)])
    near = moved(own, 0)

    scalars = jnp.stack(
        [
            side,
            jnp.where(side == 0, y, x),
            jnp.where(side == 0, x, y),
            lax.axis_index("z"),
            index,
        ]
    ).astype(jnp.int32)
    near, far, scalars = lax.optimization_barrier((near, far, scalars))
    tally = jnp.full((8, own.shape[1]), live).astype(jnp.bfloat16)
    blocks = [line_of(jnp.concatenate([near, far, tally]))]
    for step in STEPS[1:]:
        blocks.append(passed_on(blocks[0], step))
    joined, last = join(blocks[:2]), join(blocks[2:])
    mates = [(0, 1), (1, 0)]
    other_joined = lax.ppermute(joined, "core", mates)
    other_last = lax.ppermute(last, "core", mates)
    projected, before, ends = project(
        scalars, slots, left, right, doc_lengths, joined, last
    )
    return attend(
        scalars,
        pad_counts,
        range_shift,
        slots,
        left,
        right,
        projected,
        before,
        ends,
        other_joined,
        other_last,
    )[None]


def solution(mesh):
    fine = Mesh(mesh.devices.reshape(4, 4, 2, -1), ("y", "x", "core", "z"))
    in_specs = (P("z", PLANE, None), P("z", PLANE), P("z", None), P("z", None), P("z", None))
    return jax.shard_map(
        shards, mesh=fine, in_specs=in_specs, out_specs=P("z", PLANE, None), check_vma=False
    )
```
